32 devices in a mesh: gx: 8 (over y, x, core), gy: 4 (over z).
Axes of the slice: x: 2, y: 2, z: 4, core: 2. Of those that a mesh axis runs over, the one named last changes fastest.
Arguments:
- populations: float32 [19, 128, 128, 128], P(None, 'gx', 'gy'), may hold values from 0 to 10, as said below
- solid: int32 [128, 128, 128], P('gx', 'gy'), may hold values 0 or 1
Outputs:
- advanced: float32 [19, 128, 128, 128], P(None, 'gx', 'gy')
The draws below stay inside these ranges and needn't reach their ends.
Inputs may be any that keep to these rules, and one draw needn't show every extreme that they name: populations are positive, each between 0.5 w_i 18 and 1.5 w_i 18.
All inputs are finite; a program needn't handle non-finite values. No bound on the sum of `solid` on one device may be relied on, other than what follows from the above.
Results may differ from the reference program's by a relative error of at most 0.0001.
Values sent between devices are 32-bit elements; how exact they have to be, the bound alone decides.
A program may use at most 128 MiB of HBM per device.

```python
import jax
import jax.numpy as jnp
import numpy as np
from jax import lax

NZ = 128
ITERS = 3
NX = 128
NY = 128


def draw_populations(key, part):
    weights = jnp.array([1.0 / 3.0] + [1.0 / 18.0] * 6 + [1.0 / 36.0] * 12, jnp.float32)
    rough = jax.random.uniform(key, (19, NX, NY, NZ), jnp.float32, -1.0, 1.0)
    factor = 1.0 + 0.45 * rough
    return (18.0 * weights[:, None, None, None] * factor).astype(jnp.float32)


def set_ends(entries, key, least, high):
    place = [jax.random.randint(jax.random.fold_in(key, axis), (), 0, length) for axis, length in enumerate(entries.shape)]
    widest = entries.shape.index(max(entries.shape))
    beside = place[:widest] + [(place[widest] + 1) % entries.shape[widest]] + place[widest + 1:]
    return entries.at[tuple(place)].set(least).at[tuple(beside)].set(high)


def setup_inputs(seed: int = 0) -> dict:
    key_of = jax.random.split(jax.random.key(seed), 3)
    populations = draw_populations(jax.random.fold_in(key_of[2], 71), 0)
    solid = set_ends((jax.random.randint(key_of[1], (NX, NY, NZ), 0, 8) < 1).astype(jnp.int32), jax.random.fold_in(key_of[1], 1), 0, 1)
    return {"populations": populations, "solid": solid}


velocity_table = np.array([[0, 0, 0], [1, 0, 0], [-1, 0, 0], [0, 1, 0], [0, -1, 0], [0, 0, 1], [0, 0, -1], [1, 1, 0], [-1, -1, 0], [1, -1, 0], [-1, 1, 0], [1, 0, 1], [-1, 0, -1], [1, 0, -1], [-1, 0, 1], [0, 1, 1], [0, -1, -1], [0, 1, -1], [0, -1, 1]])
weight_table = np.array([1.0 / 3.0] + [1.0 / 18.0] * 6 + [1.0 / 36.0] * 12)
relax = 1.6


def opposite(index):
    if index == 0:
        return 0
    return index + 1 if index % 2 == 1 else index - 1


def collide(field, fluid):
    table = jnp.asarray(velocity_table, jnp.float32)
    weights = jnp.asarray(weight_table, jnp.float32)
    density = jnp.sum(field, axis=0)
    moment = jnp.tensordot(table.T, field, axes=1, precision=lax.Precision.HIGHEST)
    speed = moment / density
    along = jnp.tensordot(table, speed, axes=1, precision=lax.Precision.HIGHEST)
    square = jnp.sum(speed * speed, axis=0)
    balance = weights[:, None, None, None] * density * (1.0 + 3.0 * along + 4.5 * along * along - 1.5 * square)
    return jnp.where(fluid, field + relax * (balance - field), field)


def reference(populations, solid):
    fluid = solid == 0
    field = populations
    for step in range(ITERS):
        post = collide(field, fluid)
        result = []
        for index in range(19):
            shift = tuple(int(v) for v in velocity_table[index])
            source = jnp.roll(post[index], shift, axis=(0, 1, 2))
            blocked = jnp.roll(solid, shift, axis=(0, 1, 2)) != 0
            value = jnp.where(blocked, post[opposite(index)], source)
            result.append(jnp.where(fluid, value, post[index]))
        field = jnp.stack(result)
    return field
```

```python
import functools

import jax
import jax.numpy as jnp
from jax import lax
from jax.experimental import pallas as pl
from jax.experimental.pallas import tpu as pltpu
from jax.sharding import PartitionSpec as P

ITERS = 3
MESH = pl.DeviceIdType.MESH

VELOCITY = (
    (0, 0, 0),
    (1, 0, 0), (-1, 0, 0), (0, 1, 0), (0, -1, 0), (0, 0, 1), (0, 0, -1),
    (1, 1, 0), (-1, -1, 0), (1, -1, 0), (-1, 1, 0),
    (1, 0, 1), (-1, 0, -1), (1, 0, -1), (-1, 0, 1),
    (0, 1, 1), (0, -1, -1), (0, 1, -1), (0, -1, 1),
)
RELAX = 1.6
BIG = 1e37
BLOCKED = 1e34

UP_X = [1, 7, 9, 11, 13]
DOWN_X = [2, 8, 10, 12, 14]
ORDER = UP_X + DOWN_X + [0, 3, 4, 5, 6, 15, 16, 17, 18]
SLOT = {index: slot for slot, index in enumerate(ORDER)}
UP_Y = [3, 7, 10, 15, 17]
DOWN_Y = [4, 8, 9, 16, 18]
CORNERS = (7, 8, 9, 10)


def opposite(index):
    if index == 0:
        return 0
    return index + 1 if index % 2 == 1 else index - 1


def collide(f, fluid):
    total = {}
    delta = {}
    for i in range(1, 19, 2):
        total[i] = f[i] + f[i + 1]
        delta[i] = f[i] - f[i + 1]
    rho = f[0] + ((total[1] + total[3]) + (total[5] + total[7])) + (
        ((total[9] + total[11]) + (total[13] + total[15])) + total[17]
    )
    mx = (delta[1] + delta[7]) + (delta[9] + delta[11]) + delta[13]
    my = (delta[3] + delta[7]) + (delta[15] - delta[9]) + delta[17]
    mz = (delta[5] + delta[11]) + (delta[15] - delta[13]) - delta[17]
    zero = jnp.zeros_like(rho)
    scale = RELAX * 3.0 / 36.0
    mx = jnp.where(fluid, mx * scale, zero)
    my = jnp.where(fluid, my * scale, zero)
    mz = jnp.where(fluid, mz * scale, zero)
    inv = 1.0 / rho
    curve = inv * (RELAX * 4.5 / 36.0 / (scale * scale))
    base = rho * (RELAX / 36.0) - (mx * mx + my * my + mz * mz) * (
        inv * (RELAX * 1.5 / 36.0 / (scale * scale))
    )
    base = jnp.where(fluid, base, jnp.full_like(rho, BIG * RELAX / 36.0))
    post = [None] * 19
    keep = 1.0 - RELAX
    half = keep * 0.5
    post[0] = base * 12.0 + f[0] * keep
    base2 = base + base
    curve2 = curve + curve
    for i in range(1, 19, 2):
        cx, cy, cz = VELOCITY[i]
        along = None
        for c, m in ((cx, mx), (cy, my), (cz, mz)):
            if c == 0:
                continue
            if along is None:
                along = m
            else:
                along = along + m if c > 0 else along - m
        if i < 7:
            even = base2 + along * along * curve2
            odd = along + along
        else:
            even = base + along * along * curve
            odd = along
        even = even + total[i] * half
        odd = odd + delta[i] * half
        post[i] = even + odd
        post[i + 1] = even - odd
    return post


def kernel(sizes, axes, f_hbm, solid, out, field, p0, p1, p2, y_send, y_recv, in_sem, send_sem, recv_sem):
    rows, cols, gx_size, gy_size = sizes
    gx, gy = axes
    tiles = cols // 8
    buffers = (p0, p1, p2)
    me_x, me_y = lax.axis_index(gx), lax.axis_index(gy)
    up_x, down_x = lax.rem(me_x + 1, gx_size), lax.rem(me_x + gx_size - 1, gx_size)
    up_y, down_y = lax.rem(me_y + 1, gy_size), lax.rem(me_y + gy_size - 1, gy_size)
    place_x = {1: up_x, 0: me_x, -1: down_x}
    place_y = {1: up_y, 0: me_y, -1: down_y}

    def device(dx, dy):
        return {gx: place_x[dx], gy: place_y[dy]}

    inner = rows - 2
    pairs = inner // 2

    def load(start, count, sem):
        return pltpu.make_async_copy(
            f_hbm.at[:, pl.ds(start, count)], field.at[:, pl.ds(start, count)], in_sem.at[sem]
        )

    load(0, 1, 0).start()
    load(rows - 1, 1, 1).start()
    for c in range(pairs):
        load(1 + 2 * c, 2, 2 + c).start()

    barrier = pltpu.get_barrier_semaphore()
    around = [(dx, dy) for dx in (-1, 0, 1) for dy in (-1, 0, 1) if (dx, dy) != (0, 0)]
    for dx, dy in around:
        pl.semaphore_signal(barrier, inc=1, device_id=device(dx, dy), device_id_type=MESH)

    def remote(src, dst, phase, which, dx, dy):
        return pltpu.make_async_remote_copy(
            src_ref=src,
            dst_ref=dst,
            send_sem=send_sem.at[phase, which],
            recv_sem=recv_sem.at[phase, which],
            device_id=device(dx, dy),
            device_id_type=MESH,
        )

    def x_copies(phase):
        buf = buffers[phase]
        own = pl.ds(8, cols)
        copies = [
            remote(buf.at[pl.ds(0, 5), rows, own], buf.at[pl.ds(0, 5), 0, own], phase, 0, 1, 0),
            remote(buf.at[pl.ds(5, 5), 1, own], buf.at[pl.ds(5, 5), rows + 1, own], phase, 1, -1, 0),
        ]
        for k, index in enumerate(CORNERS):
            cx, cy, _ = VELOCITY[index]
            slot = SLOT[index]
            src_x, dst_x = (rows, 0) if cx > 0 else (1, rows + 1)
            src_y, dst_y = (cols, 0) if cy > 0 else (8, cols + 8)
            copies.append(
                remote(
                    buf.at[slot, src_x, pl.ds(src_y, 8)],
                    buf.at[slot, dst_x, pl.ds(dst_y, 8)],
                    phase, 4 + k, cx, cy,
                )
            )
        return copies

    def y_copies(phase):
        return [
            remote(y_send.at[phase, 0], y_recv.at[phase, 0], phase, 2, 0, 1),
            remote(y_send.at[phase, 1], y_recv.at[phase, 1], phase, 3, 0, -1),
        ]

    def pull(buf, x, t):
        top = 8 + 8 * t
        own = [buf[SLOT[i], x + 1, pl.ds(top, 8), :] for i in range(19)]
        f = [own[0]]
        for i in range(1, 19):
            cx, cy, cz = VELOCITY[i]
            if cx == 0 and cy == 0:
                value = own[i]
            else:
                value = buf[SLOT[i], x + 1 - cx, pl.ds(top - cy, 8), :]
            if cz:
                value = pltpu.roll(value, 1 if cz > 0 else value.shape[1] - 1, axis=1)
            f.append(jnp.where(value > BLOCKED, own[opposite(i)], value))
        return f

    def advance(phase, x, t):
        fluid = solid[x, pl.ds(8 * t, 8), :] == 0
        if phase == 0:
            f = [field[i, x, pl.ds(8 * t, 8), :] for i in range(19)]
        else:
            f = pull(buffers[phase - 1], x, t)
        post = collide(f, fluid)
        buf = buffers[phase]
        for i in range(19):
            buf[SLOT[i], x + 1, pl.ds(8 + 8 * t, 8), :] = post[i]
        if t == tiles - 1:
            for j, index in enumerate(UP_Y):
                y_send[phase, 0, j, pl.ds(x, 1), :] = post[index][7:8]
        if t == 0:
            for j, index in enumerate(DOWN_Y):
                y_send[phase, 1, j, pl.ds(x, 1), :] = post[index][0:1]

    def finish(x, t):
        fluid = solid[x, pl.ds(8 * t, 8), :] == 0
        f = pull(buffers[ITERS - 1], x, t)
        for i in range(19):
            kept = field[i, x, pl.ds(8 * t, 8), :]
            out[i, x, pl.ds(8 * t, 8), :] = jnp.where(fluid, f[i], kept)

    edge_tiles = sorted({0, tiles - 1})
    inner_tiles = [t for t in range(tiles) if t not in edge_tiles]

    def loop(body, which):
        if not which:
            return

        def step(c, carry):
            for dx in range(2):
                for t in which:
                    body(1 + 2 * c + dx, t)
            return carry

        lax.fori_loop(0, pairs, step, 0)

    def merge(phase):
        buf = buffers[phase]

        def step(x, carry):
            for j, index in enumerate(UP_Y):
                buf[SLOT[index], x + 1, pl.ds(7, 1), :] = y_recv[phase, 0, j, pl.ds(x, 1), :]
            for j, index in enumerate(DOWN_Y):
                buf[SLOT[index], x + 1, pl.ds(cols + 8, 1), :] = y_recv[phase, 1, j, pl.ds(x, 1), :]
            return carry

        lax.fori_loop(0, rows, step, 0)

    for phase in range(ITERS):
        if phase == 0:
            load(0, 1, 0).wait()
            load(rows - 1, 1, 1).wait()
        else:
            for copy in y_copies(phase - 1):
                copy.wait_recv()
            merge(phase - 1)
            for copy in x_copies(phase - 1):
                copy.wait_recv()
        for x in (0, rows - 1):
            for t in range(tiles):
                advance(phase, x, t)
        if phase == 0:
            pl.semaphore_wait(barrier, len(around))
        for copy in x_copies(phase):
            copy.start()
        if phase == 0:
            for c in range(pairs):
                load(1 + 2 * c, 2, 2 + c).wait()
        loop(functools.partial(advance, phase), edge_tiles)
        for copy in y_copies(phase):
            copy.start()
        loop(functools.partial(advance, phase), inner_tiles)

    loop(finish, inner_tiles)
    last = ITERS - 1
    for copy in y_copies(last):
        copy.wait_recv()
    merge(last)
    loop(finish, edge_tiles)
    for copy in x_copies(last):
        copy.wait_recv()
    for x in (0, rows - 1):
        for t in range(tiles):
            finish(x, t)
    for phase in range(ITERS):
        for copy in x_copies(phase) + y_copies(phase):
            copy.wait_send()


def solution(mesh):
    gx, gy = mesh.axis_names
    gx_size, gy_size = mesh.shape[gx], mesh.shape[gy]

    def local(populations, solid):
        count, rows, cols, lanes = populations.shape
        f32 = jnp.float32
        padded = pltpu.VMEM((count, rows + 2, cols + 16, lanes), f32)
        return pl.pallas_call(
            functools.partial(kernel, (rows, cols, gx_size, gy_size), (gx, gy)),
            out_shape=jax.ShapeDtypeStruct(populations.shape, f32),
            in_specs=[pl.BlockSpec(memory_space=pltpu.HBM), pl.BlockSpec(memory_space=pltpu.VMEM)],
            out_specs=pl.BlockSpec(memory_space=pltpu.VMEM),
            scratch_shapes=[
                pltpu.VMEM((count, rows, cols, lanes), f32),
                padded,
                padded,
                padded,
                pltpu.VMEM((ITERS, 2, 5, rows, lanes), f32),
                pltpu.VMEM((ITERS, 2, 5, rows, lanes), f32),
                pltpu.SemaphoreType.DMA((2 + (rows - 2) // 2,)),
                pltpu.SemaphoreType.DMA((ITERS, 8)),
                pltpu.SemaphoreType.DMA((ITERS, 8)),
            ],
            compiler_params=pltpu.CompilerParams(
                collective_id=0, has_side_effects=True, vmem_limit_bytes=44 * 1024 * 1024
            ),
        )(populations, solid)

    return jax.shard_map(
        local,
        mesh=mesh,
        in_specs=(P(None, gx, gy, None), P(gx, gy, None)),
        out_specs=P(None, gx, gy, None),
        check_vma=False,
    )
```

```python
import functools

import jax
import jax.numpy as jnp
from jax import lax
from jax.experimental import pallas as pl
from jax.experimental.pallas import tpu as pltpu
from jax.sharding import PartitionSpec as P

ITERS = 3
MESH = pl.DeviceIdType.MESH

VELOCITY = (
    (0, 0, 0),
    (1, 0, 0), (-1, 0, 0), (0, 1, 0), (0, -1, 0), (0, 0, 1), (0, 0, -1),
    (1, 1, 0), (-1, -1, 0), (1, -1, 0), (-1, 1, 0),
    (1, 0, 1), (-1, 0, -1), (1, 0, -1), (-1, 0, 1),
    (0, 1, 1), (0, -1, -1), (0, 1, -1), (0, -1, 1),
)
RELAX = 1.6
BIG = 1e37
BLOCKED = 1e34

UP_X = [1, 7, 9, 11, 13]
DOWN_X = [2, 8, 10, 12, 14]
ORDER = UP_X + DOWN_X + [0, 3, 4, 5, 6, 15, 16, 17, 18]
SLOT = {index: slot for slot, index in enumerate(ORDER)}
UP_Y = [3, 7, 10, 15, 17]
DOWN_Y = [4, 8, 9, 16, 18]
CORNERS = (7, 8, 9, 10)


def opposite(index):
    if index == 0:
        return 0
    return index + 1 if index % 2 == 1 else index - 1


def collide(f, fluid):
    total = {}
    delta = {}
    for i in range(1, 19, 2):
        total[i] = f[i] + f[i + 1]
        delta[i] = f[i] - f[i + 1]
    rho = f[0] + ((total[1] + total[3]) + (total[5] + total[7])) + (
        ((total[9] + total[11]) + (total[13] + total[15])) + total[17]
    )
    mx = (delta[1] + delta[7]) + (delta[9] + delta[11]) + delta[13]
    my = (delta[3] + delta[7]) + (delta[15] - delta[9]) + delta[17]
    mz = (delta[5] + delta[11]) + (delta[15] - delta[13]) - delta[17]
    zero = jnp.zeros_like(rho)
    scale = RELAX * 3.0 / 36.0
    mx = jnp.where(fluid, mx * scale, zero)
    my = jnp.where(fluid, my * scale, zero)
    mz = jnp.where(fluid, mz * scale, zero)
    inv = 1.0 / rho
    curve = inv * (RELAX * 4.5 / 36.0 / (scale * scale))
    base = rho * (RELAX / 36.0) - (mx * mx + my * my + mz * mz) * (
        inv * (RELAX * 1.5 / 36.0 / (scale * scale))
    )
    base = jnp.where(fluid, base, jnp.full_like(rho, BIG * RELAX / 36.0))
    post = [None] * 19
    keep = 1.0 - RELAX
    half = keep * 0.5
    post[0] = base * 12.0 + f[0] * keep
    base2 = base + base
    curve2 = curve + curve
    for i in range(1, 19, 2):
        cx, cy, cz = VELOCITY[i]
        along = None
        for c, m in ((cx, mx), (cy, my), (cz, mz)):
            if c == 0:
                continue
            if along is None:
                along = m
            else:
                along = along + m if c > 0 else along - m
        if i < 7:
            even = base2 + along * along * curve2
            odd = along + along
        else:
            even = base + along * along * curve
            odd = along
        even = even + total[i] * half
        odd = odd + delta[i] * half
        post[i] = even + odd
        post[i + 1] = even - odd
    return post


def kernel(sizes, axes, f_hbm, solid_hbm, out, field, solid, p0, p1, p2, y_send, y_recv, in_sem, send_sem, recv_sem):
    rows, cols, gx_size, gy_size = sizes
    gx, gy = axes
    tiles = cols // 8
    buffers = (p0, p1, p2)
    me_x, me_y = lax.axis_index(gx), lax.axis_index(gy)
    up_x, down_x = lax.rem(me_x + 1, gx_size), lax.rem(me_x + gx_size - 1, gx_size)
    up_y, down_y = lax.rem(me_y + 1, gy_size), lax.rem(me_y + gy_size - 1, gy_size)
    place_x = {1: up_x, 0: me_x, -1: down_x}
    place_y = {1: up_y, 0: me_y, -1: down_y}

    def device(dx, dy):
        return {gx: place_x[dx], gy: place_y[dy]}

    inner = rows - 2
    pairs = inner // 2
    half = rows // 2

    def load(start, count, sem):
        return pltpu.make_async_copy(
            f_hbm.at[:, pl.ds(start, count)], field.at[:, pl.ds(start, count)], in_sem.at[sem]
        )

    barrier = pltpu.get_barrier_semaphore()
    around = [(dx, dy) for dx in (-1, 0, 1) for dy in (-1, 0, 1) if (dx, dy) != (0, 0)]
    for dx, dy in around:
        pl.semaphore_signal(barrier, inc=1, device_id=device(dx, dy), device_id_type=MESH)

    load_solid = pltpu.make_async_copy(solid_hbm, solid, in_sem.at[2 + pairs])
    load_solid.start()
    load(0, 1, 0).start()
    load(rows - 1, 1, 1).start()
    for c in range(pairs):
        load(1 + 2 * c, 2, 2 + c).start()

    def remote(src, dst, phase, which, dx, dy):
        return pltpu.make_async_remote_copy(
            src_ref=src,
            dst_ref=dst,
            send_sem=send_sem.at[phase, which],
            recv_sem=recv_sem.at[phase, which],
            device_id=device(dx, dy),
            device_id_type=MESH,
        )

    def x_copies(phase, side):
        buf = buffers[phase]
        own = pl.ds(8, cols)
        src_x, dst_x, slots = (rows, 0, pl.ds(0, 5)) if side > 0 else (1, rows + 1, pl.ds(5, 5))
        copies = [
            remote(
                buf.at[slots, src_x, own], buf.at[slots, dst_x, own], phase, 0 if side > 0 else 1, side, 0
            )
        ]
        for k, index in enumerate(CORNERS):
            cx, cy, _ = VELOCITY[index]
            if cx != side:
                continue
            slot = SLOT[index]
            src_y, dst_y = (cols, 0) if cy > 0 else (8, cols + 8)
            copies.append(
                remote(
                    buf.at[slot, src_x, pl.ds(src_y, 8)],
                    buf.at[slot, dst_x, pl.ds(dst_y, 8)],
                    phase, 2 + k, cx, cy,
                )
            )
        return copies

    def y_copies(phase, chunk):
        planes = pl.ds(chunk * half, half)
        return [
            remote(
                y_send.at[phase, side, :, planes], y_recv.at[phase, side, :, planes],
                phase, 6 + 2 * side + chunk, 0, 1 - 2 * side,
            )
            for side in range(2)
        ]

    def pull(buf, x, t):
        top = 8 + 8 * t
        own = [buf[SLOT[i], x + 1, pl.ds(top, 8), :] for i in range(19)]
        f = [own[0]]
        for i in range(1, 19):
            cx, cy, cz = VELOCITY[i]
            if cx == 0 and cy == 0:
                value = own[i]
            else:
                value = buf[SLOT[i], x + 1 - cx, pl.ds(top - cy, 8), :]
            if cz:
                value = pltpu.roll(value, 1 if cz > 0 else value.shape[1] - 1, axis=1)
            f.append(jnp.where(value > BLOCKED, own[opposite(i)], value))
        return f

    def advance(phase, x, t):
        fluid = solid[x, pl.ds(8 * t, 8), :] == 0
        if phase == 0:
            f = [field[i, x, pl.ds(8 * t, 8), :] for i in range(19)]
        else:
            f = pull(buffers[phase - 1], x, t)
        post = collide(f, fluid)
        buf = buffers[phase]
        for i in range(19):
            buf[SLOT[i], x + 1, pl.ds(8 + 8 * t, 8), :] = post[i]
        if t == tiles - 1:
            for j, index in enumerate(UP_Y):
                y_send[phase, 0, j, pl.ds(x, 1), :] = post[index][7:8]
        if t == 0:
            for j, index in enumerate(DOWN_Y):
                y_send[phase, 1, j, pl.ds(x, 1), :] = post[index][0:1]

    def finish(x, t):
        fluid = solid[x, pl.ds(8 * t, 8), :] == 0
        f = pull(buffers[ITERS - 1], x, t)
        for i in range(19):
            kept = field[i, x, pl.ds(8 * t, 8), :]
            out[i, x, pl.ds(8 * t, 8), :] = jnp.where(fluid, f[i], kept)

    edge_tiles = sorted({0, tiles - 1})
    inner_tiles = [t for t in range(tiles) if t not in edge_tiles]

    def loop(body, which, first=1, stop=rows - 1):
        if not which:
            return

        def step(c, carry):
            for dx in range(2):
                for t in which:
                    body(first + 2 * c + dx, t)
            return carry

        lax.fori_loop(0, (stop - first) // 2, step, 0)

    def merge(phase, chunk):
        buf = buffers[phase]

        def step(c, carry):
            for dx in range(2):
                x = chunk * half + 2 * c + dx
                for j, index in enumerate(UP_Y):
                    buf[SLOT[index], x + 1, pl.ds(7, 1), :] = y_recv[phase, 0, j, pl.ds(x, 1), :]
                for j, index in enumerate(DOWN_Y):
                    buf[SLOT[index], x + 1, pl.ds(cols + 8, 1), :] = y_recv[phase, 1, j, pl.ds(x, 1), :]
            return carry

        lax.fori_loop(0, half // 2, step, 0)

    def plane(body, x):
        for t in range(tiles):
            body(x, t)

    def arrive(copies):
        for copy in copies:
            copy.wait_recv()

    def send(copies):
        for copy in copies:
            copy.start()

    for phase in range(ITERS):
        body = functools.partial(advance, phase)
        if phase == 0:
            load_solid.wait()
            load(0, 1, 0).wait()
            plane(body, 0)
            pl.semaphore_wait(barrier, len(around))
            send(x_copies(phase, -1))
            load(rows - 1, 1, 1).wait()
            plane(body, rows - 1)
            send(x_copies(phase, 1))
            for c in range(pairs):
                load(1 + 2 * c, 2, 2 + c).wait()
            loop(body, edge_tiles, 1, half - 1)
        else:
            arrive(y_copies(phase - 1, 0))
            merge(phase - 1, 0)
            arrive(x_copies(phase - 1, 1))
            plane(body, 0)
            send(x_copies(phase, -1))
            loop(body, edge_tiles, 1, half - 1)
            arrive(y_copies(phase - 1, 1))
            merge(phase - 1, 1)
            arrive(x_copies(phase - 1, -1))
            plane(body, rows - 1)
            send(x_copies(phase, 1))
        loop(body, edge_tiles, half - 1, half + 1)
        send(y_copies(phase, 0))
        loop(body, edge_tiles, half + 1, rows - 1)
        send(y_copies(phase, 1))
        loop(body, inner_tiles)

    last = ITERS - 1
    loop(finish, inner_tiles)
    arrive(y_copies(last, 0))
    merge(last, 0)
    arrive(x_copies(last, 1))
    plane(finish, 0)
    loop(finish, edge_tiles, 1, half - 1)
    arrive(y_copies(last, 1))
    merge(last, 1)
    loop(finish, edge_tiles, half - 1, rows - 1)
    arrive(x_copies(last, -1))
    plane(finish, rows - 1)
    for phase in range(ITERS):
        for copy in x_copies(phase, 1) + x_copies(phase, -1) + y_copies(phase, 0) + y_copies(phase, 1):
            copy.wait_send()


def solution(mesh):
    gx, gy = mesh.axis_names
    gx_size, gy_size = mesh.shape[gx], mesh.shape[gy]

    def local(populations, solid):
        count, rows, cols, lanes = populations.shape
        f32 = jnp.float32
        padded = pltpu.VMEM((count, rows + 2, cols + 16, lanes), f32)
        return pl.pallas_call(
            functools.partial(kernel, (rows, cols, gx_size, gy_size), (gx, gy)),
            out_shape=jax.ShapeDtypeStruct(populations.shape, f32),
            in_specs=[pl.BlockSpec(memory_space=pltpu.HBM)] * 2,
            out_specs=pl.BlockSpec(memory_space=pltpu.VMEM),
            scratch_shapes=[
                pltpu.VMEM((count, rows, cols, lanes), f32),
                pltpu.VMEM((rows, cols, lanes), jnp.int32),
                padded,
                padded,
                padded,
                pltpu.VMEM((ITERS, 2, 5, rows, lanes), f32),
                pltpu.VMEM((ITERS, 2, 5, rows, lanes), f32),
                pltpu.SemaphoreType.DMA((3 + (rows - 2) // 2,)),
                pltpu.SemaphoreType.DMA((ITERS, 10)),
                pltpu.SemaphoreType.DMA((ITERS, 10)),
            ],
            compiler_params=pltpu.CompilerParams(
                collective_id=0, has_side_effects=True, vmem_limit_bytes=46 * 1024 * 1024
            ),
        )(
            pltpu.with_memory_space_constraint(populations, pltpu.HBM),
            pltpu.with_memory_space_constraint(solid, pltpu.HBM),
        )

    return jax.shard_map(
        local,
        mesh=mesh,
        in_specs=(P(None, gx, gy, None), P(gx, gy, None)),
        out_specs=P(None, gx, gy, None),
        check_vma=False,
    )
```

```python
import functools

import jax
import jax.numpy as jnp
from jax import lax
from jax.experimental import pallas as pl
from jax.experimental.pallas import tpu as pltpu
from jax.sharding import PartitionSpec as P

ITERS = 3
MESH = pl.DeviceIdType.MESH

VELOCITY = (
    (0, 0, 0),
    (1, 0, 0), (-1, 0, 0), (0, 1, 0), (0, -1, 0), (0, 0, 1), (0, 0, -1),
    (1, 1, 0), (-1, -1, 0), (1, -1, 0), (-1, 1, 0),
    (1, 0, 1), (-1, 0, -1), (1, 0, -1), (-1, 0, 1),
    (0, 1, 1), (0, -1, -1), (0, 1, -1), (0, -1, 1),
)
RELAX = 1.6
BIG = 1e37
BLOCKED = 1e34

UP_X = [1, 7, 9, 11, 13]
DOWN_X = [2, 8, 10, 12, 14]
ORDER = UP_X + DOWN_X + [0, 3, 4, 5, 6, 15, 16, 17, 18]
SLOT = {index: slot for slot, index in enumerate(ORDER)}
UP_Y = [3, 7, 10, 15, 17]
DOWN_Y = [4, 8, 9, 16, 18]
CORNERS = (7, 8, 9, 10)


def opposite(index):
    if index == 0:
        return 0
    return index + 1 if index % 2 == 1 else index - 1


def collide(f, fluid):
    total = {}
    delta = {}
    for i in range(1, 19, 2):
        total[i] = f[i] + f[i + 1]
        delta[i] = f[i] - f[i + 1]
    rho = f[0] + ((total[1] + total[3]) + (total[5] + total[7])) + (
        ((total[9] + total[11]) + (total[13] + total[15])) + total[17]
    )
    mx = (delta[1] + delta[7]) + (delta[9] + delta[11]) + delta[13]
    my = (delta[3] + delta[7]) + (delta[15] - delta[9]) + delta[17]
    mz = (delta[5] + delta[11]) + (delta[15] - delta[13]) - delta[17]
    zero = jnp.zeros_like(rho)
    scale = RELAX * 3.0 / 36.0
    mx = jnp.where(fluid, mx * scale, zero)
    my = jnp.where(fluid, my * scale, zero)
    mz = jnp.where(fluid, mz * scale, zero)
    inv = 1.0 / rho
    curve = inv * (RELAX * 4.5 / 36.0 / (scale * scale))
    base = rho * (RELAX / 36.0) - (mx * mx + my * my + mz * mz) * (
        inv * (RELAX * 1.5 / 36.0 / (scale * scale))
    )
    base = jnp.where(fluid, base, jnp.full_like(rho, BIG * RELAX / 36.0))
    post = [None] * 19
    keep = 1.0 - RELAX
    half = keep * 0.5
    post[0] = base * 12.0 + f[0] * keep
    base2 = base + base
    curve2 = curve + curve
    for i in range(1, 19, 2):
        cx, cy, cz = VELOCITY[i]
        along = None
        for c, m in ((cx, mx), (cy, my), (cz, mz)):
            if c == 0:
                continue
            if along is None:
                along = m
            else:
                along = along + m if c > 0 else along - m
        if i < 7:
            even = base2 + along * along * curve2
            odd = along + along
        else:
            even = base + along * along * curve
            odd = along
        even = even + total[i] * half
        odd = odd + delta[i] * half
        post[i] = even + odd
        post[i + 1] = even - odd
    return post


def kernel(sizes, axes, f_hbm, solid_hbm, out, field, solid, p0, p1, p2, y_send, y_recv, in_sem, send_sem, recv_sem):
    rows, cols, gx_size, gy_size = sizes
    gx, gy = axes
    tiles = cols // 8
    buffers = (p0, p1, p2)
    me_x, me_y = lax.axis_index(gx), lax.axis_index(gy)
    up_x, down_x = lax.rem(me_x + 1, gx_size), lax.rem(me_x + gx_size - 1, gx_size)
    up_y, down_y = lax.rem(me_y + 1, gy_size), lax.rem(me_y + gy_size - 1, gy_size)
    place_x = {1: up_x, 0: me_x, -1: down_x}
    place_y = {1: up_y, 0: me_y, -1: down_y}

    def device(dx, dy):
        return {gx: place_x[dx], gy: place_y[dy]}

    inner = rows - 2
    pairs = inner // 2
    half = rows // 2

    def load(start, count, sem):
        return pltpu.make_async_copy(
            f_hbm.at[:, pl.ds(start, count)], field.at[:, pl.ds(start, count)], in_sem.at[sem]
        )

    barrier = pltpu.get_barrier_semaphore()
    around = [(dx, dy) for dx in (-1, 0, 1) for dy in (-1, 0, 1) if (dx, dy) != (0, 0)]
    for dx, dy in around:
        pl.semaphore_signal(barrier, inc=1, device_id=device(dx, dy), device_id_type=MESH)

    load_solid = pltpu.make_async_copy(solid_hbm, solid, in_sem.at[2 + pairs])
    load_solid.start()
    load(0, 1, 0).start()
    load(rows - 1, 1, 1).start()
    for c in range(pairs):
        load(1 + 2 * c, 2, 2 + c).start()

    def remote(src, dst, phase, which, dx, dy):
        return pltpu.make_async_remote_copy(
            src_ref=src,
            dst_ref=dst,
            send_sem=send_sem.at[phase, which],
            recv_sem=recv_sem.at[phase, which],
            device_id=device(dx, dy),
            device_id_type=MESH,
        )

    def x_copies(phase, side):
        buf = buffers[phase]
        own = pl.ds(8, cols)
        src_x, dst_x, slots = (rows, 0, pl.ds(0, 5)) if side > 0 else (1, rows + 1, pl.ds(5, 5))
        copies = [
            remote(
                buf.at[slots, src_x, own], buf.at[slots, dst_x, own], phase, 0 if side > 0 else 1, side, 0
            )
        ]
        for k, index in enumerate(CORNERS):
            cx, cy, _ = VELOCITY[index]
            if cx != side:
                continue
            slot = SLOT[index]
            src_y, dst_y = (cols, 0) if cy > 0 else (8, cols + 8)
            copies.append(
                remote(
                    buf.at[slot, src_x, pl.ds(src_y, 8)],
                    buf.at[slot, dst_x, pl.ds(dst_y, 8)],
                    phase, 2 + k, cx, cy,
                )
            )
        return copies

    def y_copies(phase, chunk):
        planes = pl.ds(chunk * half, half)
        return [
            remote(
                y_send.at[phase, side, :, planes], y_recv.at[phase, side, :, planes],
                phase, 6 + 2 * side + chunk, 0, 1 - 2 * side,
            )
            for side in range(2)
        ]

    def pull(buf, x, t):
        top = 8 + 8 * t
        own = [buf[SLOT[i], x + 1, pl.ds(top, 8), :] for i in range(19)]
        f = [own[0]]
        for i in range(1, 19):
            cx, cy, cz = VELOCITY[i]
            if cx == 0 and cy == 0:
                value = own[i]
            else:
                value = buf[SLOT[i], x + 1 - cx, pl.ds(top - cy, 8), :]
            if cz:
                value = pltpu.roll(value, 1 if cz > 0 else value.shape[1] - 1, axis=1)
            f.append(jnp.where(value > BLOCKED, own[opposite(i)], value))
        return f

    def advance(phase, x, t):
        fluid = solid[x, pl.ds(8 * t, 8), :] == 0
        if phase == 0:
            f = [field[i, x, pl.ds(8 * t, 8), :] for i in range(19)]
        else:
            f = pull(buffers[phase - 1], x, t)
        post = collide(f, fluid)
        buf = buffers[phase]
        for i in range(19):
            buf[SLOT[i], x + 1, pl.ds(8 + 8 * t, 8), :] = post[i]
        if t == tiles - 1:
            for j, index in enumerate(UP_Y):
                y_send[phase, 0, j, pl.ds(x, 1), :] = post[index][7:8]
        if t == 0:
            for j, index in enumerate(DOWN_Y):
                y_send[phase, 1, j, pl.ds(x, 1), :] = post[index][0:1]

    def finish(x, t):
        fluid = solid[x, pl.ds(8 * t, 8), :] == 0
        f = pull(buffers[ITERS - 1], x, t)
        for i in range(19):
            kept = field[i, x, pl.ds(8 * t, 8), :]
            out[i, x, pl.ds(8 * t, 8), :] = jnp.where(fluid, f[i], kept)

    edge_tiles = sorted({0, tiles - 1})
    inner_tiles = [t for t in range(tiles) if t not in edge_tiles]

    def loop(body, which, first=1, stop=rows - 1):
        if not which:
            return

        def step(c, carry):
            for dx in range(2):
                for t in which:
                    body(first + 2 * c + dx, t)
            return carry

        lax.fori_loop(0, (stop - first) // 2, step, 0)

    def merge(phase, chunk):
        buf = buffers[phase]

        def step(c, carry):
            for dx in range(2):
                x = chunk * half + 2 * c + dx
                for j, index in enumerate(UP_Y):
                    buf[SLOT[index], x + 1, pl.ds(7, 1), :] = y_recv[phase, 0, j, pl.ds(x, 1), :]
                for j, index in enumerate(DOWN_Y):
                    buf[SLOT[index], x + 1, pl.ds(cols + 8, 1), :] = y_recv[phase, 1, j, pl.ds(x, 1), :]
            return carry

        lax.fori_loop(0, half // 2, step, 0)

    def plane(body, x):
        for t in range(tiles):
            body(x, t)

    def arrive(copies):
        for copy in copies:
            copy.wait_recv()

    def send(copies):
        for copy in copies:
            copy.start()

    first_pairs = (half - 2) // 2

    def loaded(low, high):
        for c in range(low, high):
            load(1 + 2 * c, 2, 2 + c).wait()

    for phase in range(ITERS):
        body = functools.partial(advance, phase)
        if phase == 0:
            load_solid.wait()
            load(0, 1, 0).wait()
            plane(body, 0)
            pl.semaphore_wait(barrier, len(around))
            send(x_copies(phase, -1))
            load(rows - 1, 1, 1).wait()
            plane(body, rows - 1)
            send(x_copies(phase, 1))
            loaded(0, first_pairs)
            loop(body, edge_tiles, 1, half - 1)
            loaded(first_pairs, first_pairs + 1)
        else:
            arrive(y_copies(phase - 1, 0))
            merge(phase - 1, 0)
            arrive(x_copies(phase - 1, 1))
            plane(body, 0)
            send(x_copies(phase, -1))
            loop(body, edge_tiles, 1, half - 1)
            arrive(y_copies(phase - 1, 1))
            merge(phase - 1, 1)
            arrive(x_copies(phase - 1, -1))
            plane(body, rows - 1)
            send(x_copies(phase, 1))
        loop(body, edge_tiles, half - 1, half + 1)
        send(y_copies(phase, 0))
        if phase == 0:
            loaded(first_pairs + 1, pairs)
        loop(body, edge_tiles, half + 1, rows - 1)
        send(y_copies(phase, 1))
        loop(body, inner_tiles)

    last = ITERS - 1
    loop(finish, inner_tiles)
    arrive(y_copies(last, 0))
    merge(last, 0)
    arrive(x_copies(last, 1))
    plane(finish, 0)
    loop(finish, edge_tiles, 1, half - 1)
    arrive(y_copies(last, 1))
    merge(last, 1)
    loop(finish, edge_tiles, half - 1, rows - 1)
    arrive(x_copies(last, -1))
    plane(finish, rows - 1)
    for phase in range(ITERS):
        for copy in x_copies(phase, 1) + x_copies(phase, -1) + y_copies(phase, 0) + y_copies(phase, 1):
            copy.wait_send()


def solution(mesh):
    gx, gy = mesh.axis_names
    gx_size, gy_size = mesh.shape[gx], mesh.shape[gy]

    def local(populations, solid):
        count, rows, cols, lanes = populations.shape
        f32 = jnp.float32
        padded = pltpu.VMEM((count, rows + 2, cols + 16, lanes), f32)
        return pl.pallas_call(
            functools.partial(kernel, (rows, cols, gx_size, gy_size), (gx, gy)),
            out_shape=jax.ShapeDtypeStruct(populations.shape, f32),
            in_specs=[pl.BlockSpec(memory_space=pltpu.HBM)] * 2,
            out_specs=pl.BlockSpec(memory_space=pltpu.VMEM),
            scratch_shapes=[
                pltpu.VMEM((count, rows, cols, lanes), f32),
                pltpu.VMEM((rows, cols, lanes), jnp.int32),
                padded,
                padded,
                padded,
                pltpu.VMEM((ITERS, 2, 5, rows, lanes), f32),
                pltpu.VMEM((ITERS, 2, 5, rows, lanes), f32),
                pltpu.SemaphoreType.DMA((3 + (rows - 2) // 2,)),
                pltpu.SemaphoreType.DMA((ITERS, 10)),
                pltpu.SemaphoreType.DMA((ITERS, 10)),
            ],
            compiler_params=pltpu.CompilerParams(
                collective_id=0, has_side_effects=True, vmem_limit_bytes=46 * 1024 * 1024
            ),
        )(
            pltpu.with_memory_space_constraint(populations, pltpu.HBM),
            pltpu.with_memory_space_constraint(solid, pltpu.HBM),
        )

    return jax.shard_map(
        local,
        mesh=mesh,
        in_specs=(P(None, gx, gy, None), P(gx, gy, None)),
        out_specs=P(None, gx, gy, None),
        check_vma=False,
    )
```
